32 devices in a mesh: prow: 8 (over z, y), pcol: 4 (over x, core).
Axes of the slice: x: 2, y: 2, z: 4, core: 2. Of those that a mesh axis runs over, the one named last changes fastest.
Arguments:
- inverse_block: bfloat16 [2, 512, 512], P(None, 'prow', 'pcol'), may hold values from -1.75 to 1.75
- panel: bfloat16 [2, 512, 2048], P(None, ('prow', 'pcol')), may hold values from -0.5 to 0.5
- pattern: int32 [1, 4], replicated, may hold values 0 or 1
- diag_inverse: float32 [2, 512, 2048], P(None, None, 'pcol'), may hold values from -6 to 6
Outputs:
- offdiag: bfloat16 [2, 512, 2048], P(None, 'prow', 'pcol')
- diagonal: float32 [2, 512, 2048], P(None, None, 'pcol')
The draws below stay inside these ranges and needn't reach their ends.
All inputs are finite; a program needn't handle non-finite values.
Results may differ from the reference program's by a relative error of at most 0.0024.
Values may be sent and summed in bfloat16 or wider, within the bound.
No kernel may reach another device: no remote copies, remote signals or barrier semaphores. Data moves between devices by JAX's collectives and lax.ppermute only.
A program may use at most 64 MiB of HBM per device.

```python
import jax
import jax.numpy as jnp

WIDTH = 512
NSUPER = 4
ORDER = 512
COLS = 2048
ANCESTORS = 1


def touch_ends(values, stream_key, smallest, high):
    longest = values.shape.index(max(values.shape))
    spots = []
    for shift in (0, 1):
        where = [jax.random.randint(jax.random.fold_in(stream_key, axis), (), 0, length) for axis, length in enumerate(values.shape)]
        where[longest] = (where[longest] + shift) % values.shape[longest]
        spots.append(tuple(where))
    return values.at[spots[0]].set(smallest).at[spots[1]].set(high)


def level_of(stream_key, dims, pieces, low, largest):
    factor_of = 1.0
    for dim, shards_of in pieces:
        draws = jax.random.uniform(jax.random.fold_in(jax.random.fold_in(stream_key, 6), dim), (shards_of,), jnp.float32, low / len(pieces), largest / len(pieces))
        factor_of = factor_of * jnp.repeat(jnp.exp(draws), dims[dim] // shards_of).reshape((-1,) + (1,) * (len(dims) - 1 - dim))
    return factor_of


def bell_draw(rng, shape, spread, most, pieces=(), held_as=jnp.bfloat16):
    array = jax.random.normal(rng, shape, jnp.float32) * spread
    if len(pieces) > 0:
        array = level_of(rng, shape, pieces, -0.22, 0.18) * array
    return jnp.clip(array, min=-most, max=most).astype(held_as)


def setup_inputs(seed: int = 0) -> dict:
    key_list = jax.random.split(jax.random.key(seed), 5)
    inverse_block = bell_draw(key_list[0], (2, ORDER, ORDER), 0.3, 1.75, ((1, 8), (2, 4)))
    panel = bell_draw(key_list[1], (2, ORDER, COLS), (1.8 * ORDER ** -0.5), 0.5, ((1, 32),))
    pattern = touch_ends((jax.random.randint(key_list[2], (ANCESTORS, NSUPER), 0, 3) < 2).astype(jnp.int32), jax.random.fold_in(key_list[2], 1), 0, 1)
    diag_inverse = bell_draw(key_list[3], (2, WIDTH, COLS), 1.0, 6.0, ((2, 4),), jnp.float32)
    return dict(inverse_block=inverse_block, panel=panel, pattern=pattern, diag_inverse=diag_inverse)


def complex_dot(left_real, left_imag, right_real, right_imag):
    real_part = jnp.dot(left_real, right_real, preferred_element_type=jnp.float32) - jnp.dot(left_imag, right_imag, preferred_element_type=jnp.float32)
    imag_part = jnp.dot(left_real, right_imag, preferred_element_type=jnp.float32) + jnp.dot(left_imag, right_real, preferred_element_type=jnp.float32)
    return real_part, imag_part


def reference(inverse_block, panel, pattern, diag_inverse):
    row_block = jnp.arange(ORDER, dtype=jnp.int32) // WIDTH
    col_block = jnp.arange(COLS, dtype=jnp.int32) // WIDTH
    keep_mask = pattern[row_block][:, col_block]
    masked = jnp.where(keep_mask[None] > 0, panel, jnp.zeros_like(panel))
    real_part, imag_part = complex_dot(inverse_block[0], inverse_block[1], masked[0], masked[1])
    keep_float = keep_mask.astype(jnp.float32)
    coupled = (jnp.stack([real_part, imag_part]) * keep_float[None]).astype(jnp.bfloat16)
    offdiag = -coupled
    blocks = []
    for member in range(NSUPER):
        lower_real = masked[0, :, member * WIDTH:(member + 1) * WIDTH]
        lower_imag = masked[1, :, member * WIDTH:(member + 1) * WIDTH]
        upper_real = coupled[0, :, member * WIDTH:(member + 1) * WIDTH]
        upper_imag = coupled[1, :, member * WIDTH:(member + 1) * WIDTH]
        diag_real, diag_imag = complex_dot(lower_real.T, lower_imag.T, upper_real, upper_imag)
        blocks.append(jnp.stack([diag_real, diag_imag]))
    correction = jnp.concatenate(blocks, axis=2)
    return offdiag, diag_inverse + correction
```

```python
import functools

import jax
import jax.numpy as jnp
from jax import lax
from jax.experimental import pallas as pl
from jax.experimental.pallas import tpu as pltpu
from jax.sharding import PartitionSpec as P


def complex_product(left_real, left_imag, right_real, right_imag, contract):
    dims = (((contract,), (0,)), ((), ()))
    real_part = lax.dot_general(
        left_real, right_real, dims, preferred_element_type=jnp.float32
    ) - lax.dot_general(left_imag, right_imag, dims, preferred_element_type=jnp.float32)
    imag_part = lax.dot_general(
        left_real, right_imag, dims, preferred_element_type=jnp.float32
    ) + lax.dot_general(left_imag, right_real, dims, preferred_element_type=jnp.float32)
    return (real_part, imag_part)


def keep_table(pattern, row_start, row_count, col_start, col_count, block_width):
    row_ids = (row_start + jnp.arange(row_count, dtype=jnp.int32)) // block_width
    col_ids = (col_start + jnp.arange(col_count, dtype=jnp.int32)) // block_width
    row_select = (
        row_ids[:, None] == jnp.arange(pattern.shape[0], dtype=jnp.int32)[None, :]
    ).astype(jnp.float32)
    col_select = (
        col_ids[:, None] == jnp.arange(pattern.shape[1], dtype=jnp.int32)[None, :]
    ).astype(jnp.float32)
    pattern_value = pattern.astype(jnp.float32)
    row_pattern = jnp.dot(row_select, pattern_value, precision=lax.Precision.HIGHEST)
    return jnp.dot(row_pattern, col_select.T, precision=lax.Precision.HIGHEST)


def split_plan(inverse_block, panel, pattern, diag_inverse):
    WIDTH = diag_inverse.shape[1]
    rows_dev = inverse_block.shape[1]
    block_span = inverse_block.shape[2]
    fine_rows = panel.shape[1]
    columns = panel.shape[2]
    row_index = lax.axis_index("prow")
    col_index = lax.axis_index("pcol")
    col_count = lax.axis_size("pcol")
    root_count = lax.axis_size("prow") // col_count
    fine_start = (row_index * col_count + col_index) * fine_rows
    keep_mask = keep_table(pattern, fine_start, fine_rows, 0, columns, WIDTH)
    masked = jnp.where(keep_mask[None] > 0.5, panel, jnp.zeros_like(panel))
    row_panel = lax.all_gather(masked, "pcol", axis=1, tiled=True)
    flipped = jnp.swapaxes(inverse_block, 1, 2)
    split_cols = flipped.reshape(2, root_count, col_count, fine_rows, rows_dev)
    received = lax.all_to_all(split_cols, "pcol", split_axis=2, concat_axis=1, tiled=True)
    regrouped = received.reshape(2, block_span, rows_dev)
    panel_piece = lax.all_gather(masked, "prow", axis=1, tiled=True)
    part_real, part_imag = complex_product(
        regrouped[0], regrouped[1], panel_piece[0], panel_piece[1], 0
    )
    stacked = jnp.stack([part_real, part_imag])
    summed = lax.psum_scatter(stacked, "pcol", scatter_dimension=2, tiled=True)
    local_cols = summed.shape[2]
    keep_local = keep_table(
        pattern, row_index * rows_dev, rows_dev, col_index * local_cols, local_cols, WIDTH
    )
    coupled = (summed * keep_local[None]).astype(jnp.bfloat16)
    offdiag = -coupled
    block_start = col_index * local_cols // WIDTH * WIDTH
    lower_panel = lax.dynamic_slice_in_dim(row_panel, block_start, WIDTH, 2)
    diag_real, diag_imag = complex_product(
        lower_panel[0], lower_panel[1], coupled[0], coupled[1], 0
    )
    shares = lax.psum_scatter(
        jnp.stack([diag_real, diag_imag]), "prow", scatter_dimension=1, tiled=True
    )
    correction = lax.all_gather(shares, "prow", axis=1, tiled=True)
    return (offdiag, diag_inverse + correction)


def shift_perm(outer, inner, outer_step, inner_step):
    return [
        (i * inner + j, (i + outer_step) % outer * inner + (j + inner_step) % inner)
        for i in range(outer)
        for j in range(inner)
    ]


def dot(left, right, contract):
    return lax.dot_general(
        left, right, (((contract,), (0,)), ((), ())), preferred_element_type=jnp.float32
    )


def finish_kernel(
    place_ref, pattern_ref, *refs, prow, pcol, panel_count, inverse_count, width
):
    panel_refs = refs[:panel_count]
    inverse_refs = refs[panel_count : panel_count + inverse_count]
    diag_ref, offdiag_ref, out_ref, masked_ref, inv_ref, coupled_ref = refs[
        panel_count + inverse_count :
    ]
    outer, inner = prow // 2, 2
    groups = pcol // 2
    row, col = place_ref[0], place_ref[1]
    row_hi, row_lo = row // inner, row % inner
    col_hi, col_lo = col // 2, col % 2
    rows_dev = inv_ref.shape[1] // prow
    span = inv_ref.shape[2] // pcol
    fine = rows_dev // pcol
    step = pl.program_id(0)
    cols_step = out_ref.shape[2]
    block_rows = pattern_ref.shape[0]

    def source_row(dz, dy):
        return (row_hi + outer - dz) % outer * inner + (row_lo + inner - dy) % inner

    @pl.when(step == 0)
    def _():
        for dy in range(inner):
            for dz in range(outer):
                piece = panel_refs[dy * outer + dz]
                base = source_row(dz, dy) * rows_dev
                keep = pattern_ref[base // width, col * masked_ref.shape[2] // width] > 0
                for s in range(pcol):
                    at = pl.multiple_of(base + (col + pcol - s) % pcol * fine, fine)
                    values = piece[s]
                    masked_ref[:, pl.ds(at, fine), :] = jnp.where(
                        keep, values, jnp.zeros_like(values)
                    )
        pieces = []
        for ref in inverse_refs:
            pieces += [(ref, n) for n in range(ref.shape[0])]
        order = [
            (dk, dx, dy, dz)
            for dk in range(2)
            for dx in range(groups)
            for dy in range(inner)
            for dz in range(outer)
        ]
        for (ref, n), (dk, dx, dy, dz) in zip(pieces, order, strict=True):
            at_row = pl.multiple_of(source_row(dz, dy) * rows_dev, rows_dev)
            source_col = (col_hi + groups - dx) % groups * 2 + (col_lo + 2 - dk) % 2
            at_col = pl.multiple_of(source_col * span, span)
            inv_ref[:, pl.ds(at_row, rows_dev), pl.ds(at_col, span)] = ref[n]

    here = pl.ds(pl.multiple_of(step * cols_step, cols_step), cols_step)
    right_real, right_imag = masked_ref[0, :, here], masked_ref[1, :, here]
    parts = (
        dot(inv_ref[0], right_real, 1) - dot(inv_ref[1], right_imag, 1),
        dot(inv_ref[0], right_imag, 1) + dot(inv_ref[1], right_real, 1),
    )
    for part, values in enumerate(parts):
        for block in range(block_rows):
            keep = pattern_ref[block, col * masked_ref.shape[2] // width] > 0
            rows = values[block * width : (block + 1) * width]
            coupled_ref[part, block * width : (block + 1) * width, :] = jnp.where(
                keep, rows, jnp.zeros_like(rows)
            ).astype(coupled_ref.dtype)
    own = pl.ds(pl.multiple_of(row * rows_dev, rows_dev), rows_dev)
    offdiag_ref[...] = -coupled_ref[:, own, :]
    real, imag = coupled_ref[0], coupled_ref[1]
    left_real, left_imag = masked_ref[0], masked_ref[1]
    out_ref[0] = diag_ref[0] + (dot(left_real, real, 0) - dot(left_imag, imag, 0))
    out_ref[1] = diag_ref[1] + (dot(left_real, imag, 0) + dot(left_imag, real, 0))


def copy_plan(inverse_block, panel, pattern, diag_inverse):
    row = lax.axis_index("prow")
    col = lax.axis_index("pcol")
    prow = lax.axis_size("prow")
    pcol = lax.axis_size("pcol")
    width = diag_inverse.shape[1]
    local_cols = diag_inverse.shape[2]
    parts, rows_dev, span = inverse_block.shape
    outer, inner, groups = prow // 2, 2, pcol // 2

    inv_own = inverse_block[None]
    inv_far = [
        lax.ppermute(inv_own, "prow", shift_perm(outer, inner, dz, 0)) for dz in range(1, outer)
    ]
    fine_pieces = []
    for s in range(pcol):
        at = (col + s) % pcol * local_cols
        piece = lax.dynamic_slice_in_dim(panel, at, local_cols, 2)
        if s:
            piece = lax.ppermute(piece, "pcol", shift_perm(pcol, 1, s, 0))
        fine_pieces.append(piece)
    mine = jnp.stack(fine_pieces)
    far = [mine] + [
        lax.ppermute(mine, "prow", shift_perm(outer, inner, dz, 0)) for dz in range(1, outer)
    ]
    near = [lax.ppermute(piece, "prow", shift_perm(outer, inner, 0, 1)) for piece in far]
    panel_pieces = far + near

    inv_pieces = [jnp.concatenate([inv_own] + inv_far)]
    inv_pieces.append(lax.ppermute(inv_pieces[0], "prow", shift_perm(outer, inner, 0, 1)))
    rows_all = jnp.concatenate(inv_pieces)
    across = [rows_all] + [
        lax.ppermute(rows_all, "pcol", shift_perm(groups, 2, dx, 0)) for dx in range(1, groups)
    ]
    half = jnp.concatenate(across)
    other = lax.ppermute(half, "pcol", shift_perm(groups, 2, 0, 1))
    inverse_pieces = [half, other]

    order = prow * rows_dev
    steps = 2
    cols_step = local_cols // steps
    smem = pl.BlockSpec(memory_space=pltpu.SMEM)
    vmem = pl.BlockSpec(memory_space=pltpu.VMEM)
    diag_spec = pl.BlockSpec((parts, width, cols_step), lambda i: (0, 0, i))
    off_spec = pl.BlockSpec((parts, rows_dev, cols_step), lambda i: (0, 0, i))
    kernel = functools.partial(
        finish_kernel,
        prow=prow,
        pcol=pcol,
        panel_count=len(panel_pieces),
        inverse_count=len(inverse_pieces),
        width=width,
    )
    return pl.pallas_call(
        kernel,
        grid=(steps,),
        in_specs=[smem, smem] + [vmem] * (len(panel_pieces) + len(inverse_pieces)) + [diag_spec],
        out_specs=[off_spec, diag_spec],
        out_shape=[
            jax.ShapeDtypeStruct((parts, rows_dev, local_cols), panel.dtype),
            jax.ShapeDtypeStruct(diag_inverse.shape, diag_inverse.dtype),
        ],
        scratch_shapes=[
            pltpu.VMEM((parts, order, local_cols), panel.dtype),
            pltpu.VMEM((parts, order, pcol * span), panel.dtype),
            pltpu.VMEM((parts, order, cols_step), panel.dtype),
        ],
        compiler_params=pltpu.CompilerParams(dimension_semantics=("arbitrary",)),
        name="finish",
    )(jnp.stack([row, col]), pattern, *panel_pieces, *inverse_pieces, diag_inverse)


def local(inverse_block, panel, pattern, diag_inverse):
    prow = lax.axis_size("prow")
    pcol = lax.axis_size("pcol")
    parts, rows_dev, span = inverse_block.shape
    gathered = (rows_dev * prow) * (span * pcol + diag_inverse.shape[2]) * parts * 2
    room = gathered <= diag_inverse.size * 4 * 4
    whole_blocks = diag_inverse.shape[1] == diag_inverse.shape[2]
    even = prow % 2 == 0 and pcol % 2 == 0
    if room and whole_blocks and even:
        return copy_plan(inverse_block, panel, pattern, diag_inverse)
    return split_plan(inverse_block, panel, pattern, diag_inverse)


def solution(mesh):
    in_specs = (
        P(None, "prow", "pcol"),
        P(None, ("prow", "pcol"), None),
        P(),
        P(None, None, "pcol"),
    )
    out_specs = (P(None, "prow", "pcol"), P(None, None, "pcol"))
    return jax.shard_map(local, mesh=mesh, in_specs=in_specs, out_specs=out_specs, check_vma=False)
```

```python
import functools

import jax
import jax.numpy as jnp
from jax import lax
from jax.experimental import pallas as pl
from jax.experimental.pallas import tpu as pltpu
from jax.sharding import PartitionSpec as P


def complex_product(left_real, left_imag, right_real, right_imag, contract):
    dims = (((contract,), (0,)), ((), ()))
    real_part = lax.dot_general(
        left_real, right_real, dims, preferred_element_type=jnp.float32
    ) - lax.dot_general(left_imag, right_imag, dims, preferred_element_type=jnp.float32)
    imag_part = lax.dot_general(
        left_real, right_imag, dims, preferred_element_type=jnp.float32
    ) + lax.dot_general(left_imag, right_real, dims, preferred_element_type=jnp.float32)
    return (real_part, imag_part)


def keep_table(pattern, row_start, row_count, col_start, col_count, block_width):
    row_ids = (row_start + jnp.arange(row_count, dtype=jnp.int32)) // block_width
    col_ids = (col_start + jnp.arange(col_count, dtype=jnp.int32)) // block_width
    row_select = (
        row_ids[:, None] == jnp.arange(pattern.shape[0], dtype=jnp.int32)[None, :]
    ).astype(jnp.float32)
    col_select = (
        col_ids[:, None] == jnp.arange(pattern.shape[1], dtype=jnp.int32)[None, :]
    ).astype(jnp.float32)
    pattern_value = pattern.astype(jnp.float32)
    row_pattern = jnp.dot(row_select, pattern_value, precision=lax.Precision.HIGHEST)
    return jnp.dot(row_pattern, col_select.T, precision=lax.Precision.HIGHEST)


def split_plan(inverse_block, panel, pattern, diag_inverse):
    WIDTH = diag_inverse.shape[1]
    rows_dev = inverse_block.shape[1]
    block_span = inverse_block.shape[2]
    fine_rows = panel.shape[1]
    columns = panel.shape[2]
    row_index = lax.axis_index("prow")
    col_index = lax.axis_index("pcol")
    col_count = lax.axis_size("pcol")
    root_count = lax.axis_size("prow") // col_count
    fine_start = (row_index * col_count + col_index) * fine_rows
    keep_mask = keep_table(pattern, fine_start, fine_rows, 0, columns, WIDTH)
    masked = jnp.where(keep_mask[None] > 0.5, panel, jnp.zeros_like(panel))
    row_panel = lax.all_gather(masked, "pcol", axis=1, tiled=True)
    flipped = jnp.swapaxes(inverse_block, 1, 2)
    split_cols = flipped.reshape(2, root_count, col_count, fine_rows, rows_dev)
    received = lax.all_to_all(split_cols, "pcol", split_axis=2, concat_axis=1, tiled=True)
    regrouped = received.reshape(2, block_span, rows_dev)
    panel_piece = lax.all_gather(masked, "prow", axis=1, tiled=True)
    part_real, part_imag = complex_product(
        regrouped[0], regrouped[1], panel_piece[0], panel_piece[1], 0
    )
    stacked = jnp.stack([part_real, part_imag])
    summed = lax.psum_scatter(stacked, "pcol", scatter_dimension=2, tiled=True)
    local_cols = summed.shape[2]
    keep_local = keep_table(
        pattern, row_index * rows_dev, rows_dev, col_index * local_cols, local_cols, WIDTH
    )
    coupled = (summed * keep_local[None]).astype(jnp.bfloat16)
    offdiag = -coupled
    block_start = col_index * local_cols // WIDTH * WIDTH
    lower_panel = lax.dynamic_slice_in_dim(row_panel, block_start, WIDTH, 2)
    diag_real, diag_imag = complex_product(
        lower_panel[0], lower_panel[1], coupled[0], coupled[1], 0
    )
    shares = lax.psum_scatter(
        jnp.stack([diag_real, diag_imag]), "prow", scatter_dimension=1, tiled=True
    )
    correction = lax.all_gather(shares, "prow", axis=1, tiled=True)
    return (offdiag, diag_inverse + correction)


def shift_perm(outer, inner, outer_step, inner_step):
    return [
        (i * inner + j, (i + outer_step) % outer * inner + (j + inner_step) % inner)
        for i in range(outer)
        for j in range(inner)
    ]


def dot(left, right, contract):
    return lax.dot_general(
        left, right, (((contract,), (0,)), ((), ())), preferred_element_type=jnp.float32
    )


def finish_kernel(
    place_ref, pattern_ref, *refs, prow, pcol, panel_count, inverse_count, width
):
    panel_refs = refs[:panel_count]
    inverse_refs = refs[panel_count : panel_count + inverse_count]
    diag_ref, offdiag_ref, out_ref, masked_ref, inv_ref, coupled_ref = refs[
        panel_count + inverse_count :
    ]
    outer, inner = prow // 2, 2
    groups = pcol // 2
    row, col = place_ref[0], place_ref[1]
    row_hi, row_lo = row // inner, row % inner
    col_hi, col_lo = col // 2, col % 2
    rows_dev = inv_ref.shape[1] // prow
    span = inv_ref.shape[2] // pcol
    fine = rows_dev // pcol
    step = pl.program_id(0)
    cols_step = out_ref.shape[2]
    block_rows = pattern_ref.shape[0]

    def source_row(dz, dy):
        return (row_hi + outer - dz) % outer * inner + (row_lo + inner - dy) % inner

    @pl.when(step == 0)
    def _():
        for dy in range(inner):
            for dz in range(outer):
                piece = panel_refs[dy * outer + dz]
                base = source_row(dz, dy) * rows_dev
                keep = pattern_ref[base // width, col * masked_ref.shape[2] // width] > 0
                for s in range(pcol):
                    at = pl.multiple_of(base + (col + pcol - s) % pcol * fine, fine)
                    values = piece[s]
                    masked_ref[:, pl.ds(at, fine), :] = jnp.where(
                        keep, values, jnp.zeros_like(values)
                    )
        pieces = []
        for ref in inverse_refs:
            pieces += [(ref, n) for n in range(ref.shape[0])]
        order = [
            (dk, dx, dy, dz)
            for dk in range(2)
            for dx in range(groups)
            for dy in range(inner)
            for dz in range(outer)
        ]
        for (ref, n), (dk, dx, dy, dz) in zip(pieces, order, strict=True):
            at_row = pl.multiple_of(source_row(dz, dy) * rows_dev, rows_dev)
            source_col = (col_hi + groups - dx) % groups * 2 + (col_lo + 2 - dk) % 2
            at_col = pl.multiple_of(source_col * span, span)
            inv_ref[:, pl.ds(at_row, rows_dev), pl.ds(at_col, span)] = ref[n]

    here = pl.ds(pl.multiple_of(step * cols_step, cols_step), cols_step)
    right_real, right_imag = masked_ref[0, :, here], masked_ref[1, :, here]
    parts = (
        dot(inv_ref[0], right_real, 1) - dot(inv_ref[1], right_imag, 1),
        dot(inv_ref[0], right_imag, 1) + dot(inv_ref[1], right_real, 1),
    )
    for part, values in enumerate(parts):
        for block in range(block_rows):
            keep = pattern_ref[block, col * masked_ref.shape[2] // width] > 0
            rows = values[block * width : (block + 1) * width]
            coupled_ref[part, block * width : (block + 1) * width, :] = jnp.where(
                keep, rows, jnp.zeros_like(rows)
            ).astype(coupled_ref.dtype)
    own = pl.ds(pl.multiple_of(row * rows_dev, rows_dev), rows_dev)
    offdiag_ref[...] = -coupled_ref[:, own, :]
    real, imag = coupled_ref[0], coupled_ref[1]
    left_real, left_imag = masked_ref[0], masked_ref[1]
    out_ref[0] = diag_ref[0] + (dot(left_real, real, 0) - dot(left_imag, imag, 0))
    out_ref[1] = diag_ref[1] + (dot(left_real, imag, 0) + dot(left_imag, real, 0))


def copy_plan(inverse_block, panel, pattern, diag_inverse):
    row = lax.axis_index("prow")
    col = lax.axis_index("pcol")
    prow = lax.axis_size("prow")
    pcol = lax.axis_size("pcol")
    width = diag_inverse.shape[1]
    local_cols = diag_inverse.shape[2]
    parts, rows_dev, span = inverse_block.shape
    outer, inner, groups = prow // 2, 2, pcol // 2

    fine_pieces = [
        lax.dynamic_slice_in_dim(panel, (col + s) % pcol * local_cols, local_cols, 2)
        for s in range(pcol)
    ]
    for s in range(1, pcol):
        fine_pieces[s] = lax.ppermute(fine_pieces[s], "pcol", shift_perm(pcol, 1, s, 0))
    mine = jnp.stack(fine_pieces)
    far = [mine] + [
        lax.ppermute(mine, "prow", shift_perm(outer, inner, dz, 0)) for dz in range(1, outer)
    ]
    near = [lax.ppermute(piece, "prow", shift_perm(outer, inner, 0, 1)) for piece in far]
    panel_pieces = far + near

    inv_own = inverse_block[None]
    column = jnp.concatenate(
        [inv_own]
        + [lax.ppermute(inv_own, "prow", shift_perm(outer, inner, dz, 0)) for dz in range(1, outer)]
    )
    rows_all = [column, lax.ppermute(column, "prow", shift_perm(outer, inner, 0, 1))]
    half = list(rows_all)
    for dx in range(1, groups):
        for piece in rows_all:
            half.append(lax.ppermute(piece, "pcol", shift_perm(groups, 2, dx, 0)))
    other = [lax.ppermute(piece, "pcol", shift_perm(groups, 2, 0, 1)) for piece in half]
    inverse_pieces = half + other

    panel_pieces = [pltpu.with_memory_space_constraint(p, pltpu.VMEM) for p in panel_pieces]
    inverse_pieces = [pltpu.with_memory_space_constraint(p, pltpu.VMEM) for p in inverse_pieces]
    order = prow * rows_dev
    steps = 2
    cols_step = local_cols // steps
    smem = pl.BlockSpec(memory_space=pltpu.SMEM)
    vmem = pl.BlockSpec(memory_space=pltpu.VMEM)
    diag_spec = pl.BlockSpec((parts, width, cols_step), lambda i: (0, 0, i))
    off_spec = pl.BlockSpec((parts, rows_dev, cols_step), lambda i: (0, 0, i))
    kernel = functools.partial(
        finish_kernel,
        prow=prow,
        pcol=pcol,
        panel_count=len(panel_pieces),
        inverse_count=len(inverse_pieces),
        width=width,
    )
    return pl.pallas_call(
        kernel,
        grid=(steps,),
        in_specs=[smem, smem] + [vmem] * (len(panel_pieces) + len(inverse_pieces)) + [diag_spec],
        out_specs=[off_spec, diag_spec],
        out_shape=[
            jax.ShapeDtypeStruct((parts, rows_dev, local_cols), panel.dtype),
            jax.ShapeDtypeStruct(diag_inverse.shape, diag_inverse.dtype),
        ],
        scratch_shapes=[
            pltpu.VMEM((parts, order, local_cols), panel.dtype),
            pltpu.VMEM((parts, order, pcol * span), panel.dtype),
            pltpu.VMEM((parts, order, cols_step), panel.dtype),
        ],
        compiler_params=pltpu.CompilerParams(dimension_semantics=("arbitrary",)),
        name="finish",
    )(jnp.stack([row, col]), pattern, *panel_pieces, *inverse_pieces, diag_inverse)


def local(inverse_block, panel, pattern, diag_inverse):
    prow = lax.axis_size("prow")
    pcol = lax.axis_size("pcol")
    parts, rows_dev, span = inverse_block.shape
    gathered = (rows_dev * prow) * (span * pcol + diag_inverse.shape[2]) * parts * 2
    room = gathered <= diag_inverse.size * 4 * 4
    whole_blocks = diag_inverse.shape[1] == diag_inverse.shape[2]
    even = prow % 2 == 0 and pcol % 2 == 0
    if room and whole_blocks and even:
        return copy_plan(inverse_block, panel, pattern, diag_inverse)
    return split_plan(inverse_block, panel, pattern, diag_inverse)


def solution(mesh):
    in_specs = (
        P(None, "prow", "pcol"),
        P(None, ("prow", "pcol"), None),
        P(),
        P(None, None, "pcol"),
    )
    out_specs = (P(None, "prow", "pcol"), P(None, None, "pcol"))
    return jax.shard_map(
        local, mesh=mesh, in_specs=in_specs, out_specs=out_specs, check_vma=False
    )
```

```python
import functools

import jax
import jax.numpy as jnp
from jax import lax
from jax.experimental import pallas as pl
from jax.experimental.pallas import tpu as pltpu
from jax.sharding import PartitionSpec as P


def complex_product(left_real, left_imag, right_real, right_imag, contract):
    dims = (((contract,), (0,)), ((), ()))
    real_part = lax.dot_general(
        left_real, right_real, dims, preferred_element_type=jnp.float32
    ) - lax.dot_general(left_imag, right_imag, dims, preferred_element_type=jnp.float32)
    imag_part = lax.dot_general(
        left_real, right_imag, dims, preferred_element_type=jnp.float32
    ) + lax.dot_general(left_imag, right_real, dims, preferred_element_type=jnp.float32)
    return (real_part, imag_part)


def keep_table(pattern, row_start, row_count, col_start, col_count, block_width):
    row_ids = (row_start + jnp.arange(row_count, dtype=jnp.int32)) // block_width
    col_ids = (col_start + jnp.arange(col_count, dtype=jnp.int32)) // block_width
    row_select = (
        row_ids[:, None] == jnp.arange(pattern.shape[0], dtype=jnp.int32)[None, :]
    ).astype(jnp.float32)
    col_select = (
        col_ids[:, None] == jnp.arange(pattern.shape[1], dtype=jnp.int32)[None, :]
    ).astype(jnp.float32)
    pattern_value = pattern.astype(jnp.float32)
    row_pattern = jnp.dot(row_select, pattern_value, precision=lax.Precision.HIGHEST)
    return jnp.dot(row_pattern, col_select.T, precision=lax.Precision.HIGHEST)


def split_plan(inverse_block, panel, pattern, diag_inverse):
    WIDTH = diag_inverse.shape[1]
    rows_dev = inverse_block.shape[1]
    block_span = inverse_block.shape[2]
    fine_rows = panel.shape[1]
    columns = panel.shape[2]
    row_index = lax.axis_index("prow")
    col_index = lax.axis_index("pcol")
    col_count = lax.axis_size("pcol")
    root_count = lax.axis_size("prow") // col_count
    fine_start = (row_index * col_count + col_index) * fine_rows
    keep_mask = keep_table(pattern, fine_start, fine_rows, 0, columns, WIDTH)
    masked = jnp.where(keep_mask[None] > 0.5, panel, jnp.zeros_like(panel))
    row_panel = lax.all_gather(masked, "pcol", axis=1, tiled=True)
    flipped = jnp.swapaxes(inverse_block, 1, 2)
    split_cols = flipped.reshape(2, root_count, col_count, fine_rows, rows_dev)
    received = lax.all_to_all(split_cols, "pcol", split_axis=2, concat_axis=1, tiled=True)
    regrouped = received.reshape(2, block_span, rows_dev)
    panel_piece = lax.all_gather(masked, "prow", axis=1, tiled=True)
    part_real, part_imag = complex_product(
        regrouped[0], regrouped[1], panel_piece[0], panel_piece[1], 0
    )
    stacked = jnp.stack([part_real, part_imag])
    summed = lax.psum_scatter(stacked, "pcol", scatter_dimension=2, tiled=True)
    local_cols = summed.shape[2]
    keep_local = keep_table(
        pattern, row_index * rows_dev, rows_dev, col_index * local_cols, local_cols, WIDTH
    )
    coupled = (summed * keep_local[None]).astype(jnp.bfloat16)
    offdiag = -coupled
    block_start = col_index * local_cols // WIDTH * WIDTH
    lower_panel = lax.dynamic_slice_in_dim(row_panel, block_start, WIDTH, 2)
    diag_real, diag_imag = complex_product(
        lower_panel[0], lower_panel[1], coupled[0], coupled[1], 0
    )
    shares = lax.psum_scatter(
        jnp.stack([diag_real, diag_imag]), "prow", scatter_dimension=1, tiled=True
    )
    correction = lax.all_gather(shares, "prow", axis=1, tiled=True)
    return (offdiag, diag_inverse + correction)


def is_power(count):
    return count & (count - 1) == 0


def step_from(place, step, count):
    if is_power(count):
        return place ^ step
    return (place + count - step) % count


def step_to(place, step, count):
    if is_power(count):
        return place ^ step
    return (place + step) % count


def step_perm(outer, inner, outer_step, inner_step):
    return [
        (i * inner + j, step_to(i, outer_step, outer) * inner + step_to(j, inner_step, inner))
        for i in range(outer)
        for j in range(inner)
    ]


def dot(left, right, contract):
    return lax.dot_general(
        left, right, (((contract,), (0,)), ((), ())), preferred_element_type=jnp.float32
    )


def finish_kernel(
    row_ref, col_ref, pattern_ref, *refs, prow, pcol, panel_count, inverse_count, width
):
    panel_refs = refs[:panel_count]
    inverse_refs = refs[panel_count : panel_count + inverse_count]
    diag_ref, offdiag_ref, out_ref, masked_ref, turned_ref, inv_ref, coupled_ref = refs[
        panel_count + inverse_count :
    ]
    outer, inner = prow // 2, 2
    groups = pcol // 2
    row, col = row_ref[0], col_ref[0]
    row_hi, row_lo = row // inner, row % inner
    col_hi, col_lo = col // 2, col % 2
    rows_dev = inv_ref.shape[1] // prow
    span = inv_ref.shape[2] // pcol
    fine = rows_dev // pcol
    step = pl.program_id(0)
    cols_step = out_ref.shape[2]
    block_rows = pattern_ref.shape[0]

    def source_row(dz, dy):
        return step_from(row_hi, dz, outer) * inner + step_from(row_lo, dy, inner)

    @pl.when(step == 0)
    def _():
        for dy in range(inner):
            for dz in range(outer):
                piece = panel_refs[dy * outer + dz]
                base = source_row(dz, dy) * rows_dev
                keep = pattern_ref[base // width, col * masked_ref.shape[2] // width] > 0
                for s in range(pcol):
                    at = pl.multiple_of(base + step_from(col, s, pcol) * fine, fine)
                    values = piece[s]
                    masked_ref[:, pl.ds(at, fine), :] = jnp.where(
                        keep, values, jnp.zeros_like(values)
                    )
        pieces = []
        for ref in inverse_refs:
            pieces += [(ref, n) for n in range(ref.shape[0])]
        order = [
            (dk, dx, dy, dz)
            for dk in range(2)
            for dx in range(groups)
            for dy in range(inner)
            for dz in range(outer)
        ]
        for (ref, n), (dk, dx, dy, dz) in zip(pieces, order, strict=True):
            at_row = pl.multiple_of(source_row(dz, dy) * rows_dev, rows_dev)
            source_col = step_from(col_hi, dx, groups) * 2 + step_from(col_lo, dk, 2)
            at_col = pl.multiple_of(source_col * span, span)
            inv_ref[:, pl.ds(at_row, rows_dev), pl.ds(at_col, span)] = ref[n]
        for part in range(2):
            turned_ref[part] = masked_ref[part].T

    here = pl.ds(pl.multiple_of(step * cols_step, cols_step), cols_step)
    right_real, right_imag = masked_ref[0, :, here], masked_ref[1, :, here]
    parts = (
        dot(inv_ref[0], right_real, 1) - dot(inv_ref[1], right_imag, 1),
        dot(inv_ref[0], right_imag, 1) + dot(inv_ref[1], right_real, 1),
    )
    for part, values in enumerate(parts):
        for block in range(block_rows):
            keep = pattern_ref[block, col * masked_ref.shape[2] // width] > 0
            rows = values[block * width : (block + 1) * width]
            coupled_ref[part, block * width : (block + 1) * width, :] = jnp.where(
                keep, rows, jnp.zeros_like(rows)
            ).astype(coupled_ref.dtype)
    own = pl.ds(pl.multiple_of(row * rows_dev, rows_dev), rows_dev)
    offdiag_ref[...] = -coupled_ref[:, own, :]
    real, imag = coupled_ref[0], coupled_ref[1]
    left_real, left_imag = turned_ref[0], turned_ref[1]
    out_ref[0] = diag_ref[0] + (dot(left_real, real, 1) - dot(left_imag, imag, 1))
    out_ref[1] = diag_ref[1] + (dot(left_real, imag, 1) + dot(left_imag, real, 1))


def copy_plan(inverse_block, panel, pattern, diag_inverse):
    row = lax.axis_index("prow")
    col = lax.axis_index("pcol")
    prow = lax.axis_size("prow")
    pcol = lax.axis_size("pcol")
    width = diag_inverse.shape[1]
    local_cols = diag_inverse.shape[2]
    parts, rows_dev, span = inverse_block.shape
    outer, inner, groups = prow // 2, 2, pcol // 2

    fine_pieces = [
        lax.dynamic_slice_in_dim(panel, step_to(col, s, pcol) * local_cols, local_cols, 2)
        for s in range(pcol)
    ]
    for s in range(1, pcol):
        fine_pieces[s] = lax.ppermute(fine_pieces[s], "pcol", step_perm(pcol, 1, s, 0))
    mine = jnp.stack(fine_pieces)
    far = [mine] + [
        lax.ppermute(mine, "prow", step_perm(outer, inner, dz, 0)) for dz in range(1, outer)
    ]
    near = [lax.ppermute(piece, "prow", step_perm(outer, inner, 0, 1)) for piece in far]
    panel_pieces = far + near

    inv_own = inverse_block[None]
    column = jnp.concatenate(
        [inv_own]
        + [lax.ppermute(inv_own, "prow", step_perm(outer, inner, dz, 0)) for dz in range(1, outer)]
    )
    rows_all = [column, lax.ppermute(column, "prow", step_perm(outer, inner, 0, 1))]
    half = list(rows_all)
    for dx in range(1, groups):
        for piece in rows_all:
            half.append(lax.ppermute(piece, "pcol", step_perm(groups, 2, dx, 0)))
    other = [lax.ppermute(piece, "pcol", step_perm(groups, 2, 0, 1)) for piece in half]
    inverse_pieces = half + other

    panel_pieces = [pltpu.with_memory_space_constraint(p, pltpu.VMEM) for p in panel_pieces]
    inverse_pieces = [pltpu.with_memory_space_constraint(p, pltpu.VMEM) for p in inverse_pieces]
    order = prow * rows_dev
    steps = local_cols // 128
    cols_step = local_cols // steps
    smem = pl.BlockSpec(memory_space=pltpu.SMEM)
    vmem = pl.BlockSpec(memory_space=pltpu.VMEM)
    diag_spec = pl.BlockSpec((parts, width, cols_step), lambda i: (0, 0, i))
    off_spec = pl.BlockSpec((parts, rows_dev, cols_step), lambda i: (0, 0, i))
    kernel = functools.partial(
        finish_kernel,
        prow=prow,
        pcol=pcol,
        panel_count=len(panel_pieces),
        inverse_count=len(inverse_pieces),
        width=width,
    )
    return pl.pallas_call(
        kernel,
        grid=(steps,),
        in_specs=[smem, smem, smem] + [vmem] * (len(panel_pieces) + len(inverse_pieces)) + [diag_spec],
        out_specs=[off_spec, diag_spec],
        out_shape=[
            jax.ShapeDtypeStruct((parts, rows_dev, local_cols), panel.dtype),
            jax.ShapeDtypeStruct(diag_inverse.shape, diag_inverse.dtype),
        ],
        scratch_shapes=[
            pltpu.VMEM((parts, order, local_cols), panel.dtype),
            pltpu.VMEM((parts, local_cols, order), panel.dtype),
            pltpu.VMEM((parts, order, pcol * span), panel.dtype),
            pltpu.VMEM((parts, order, cols_step), panel.dtype),
        ],
        compiler_params=pltpu.CompilerParams(dimension_semantics=("arbitrary",)),
        name="finish",
    )(row.reshape(1), col.reshape(1), pattern, *panel_pieces, *inverse_pieces, diag_inverse)


def local(inverse_block, panel, pattern, diag_inverse):
    prow = lax.axis_size("prow")
    pcol = lax.axis_size("pcol")
    parts, rows_dev, span = inverse_block.shape
    gathered = (rows_dev * prow) * (span * pcol + diag_inverse.shape[2]) * parts * 2
    room = gathered <= diag_inverse.size * 4 * 4
    aligned = diag_inverse.shape[1] % rows_dev == 0 and rows_dev % (16 * pcol) == 0
    aligned = aligned and span % 128 == 0 and diag_inverse.shape[2] % 128 == 0
    whole_blocks = diag_inverse.shape[1] == diag_inverse.shape[2]
    even = prow % 2 == 0 and pcol % 2 == 0
    if room and whole_blocks and even and aligned:
        return copy_plan(inverse_block, panel, pattern, diag_inverse)
    return split_plan(inverse_block, panel, pattern, diag_inverse)


def solution(mesh):
    in_specs = (
        P(None, "prow", "pcol"),
        P(None, ("prow", "pcol"), None),
        P(),
        P(None, None, "pcol"),
    )
    out_specs = (P(None, "prow", "pcol"), P(None, None, "pcol"))
    return jax.shard_map(
        local, mesh=mesh, in_specs=in_specs, out_specs=out_specs, check_vma=False
    )
```
